32 devices in a mesh: seq: 16 (over z, y, x), batch: 2 (over core).
Axes of the slice: x: 2, y: 2, z: 4, core: 2. Of those that a mesh axis runs over, the one named last changes fastest.
Arguments:
- inputs: bfloat16 [2, 2048, 2048], P('batch', 'seq'), may hold values from -6 to 6
- cotangent: bfloat16 [2, 2048, 1024], P('batch', 'seq'), may hold values from -48 to 48
- w_query: bfloat16 [2048, 128], replicated, may hold values from -0.125 to 0.125
- w_key: bfloat16 [2048, 128], replicated, may hold values from -0.125 to 0.125
- w_value: bfloat16 [2048, 1024], replicated, may hold values from -0.125 to 0.125
Outputs:
- grad_inputs: bfloat16 [2, 2048, 2048], P('batch', 'seq')
- grad_w_query: float32 [2048, 128], P(('seq', 'batch'))
- grad_w_key: float32 [2048, 128], P(('seq', 'batch'))
- grad_w_value: float32 [2048, 1024], P(('seq', 'batch'))
The draws below stay inside these ranges and needn't reach their ends.
All inputs are finite; a program needn't handle non-finite values.
Results may differ from the reference program's by a relative error of at most 0.006.
Values sent between devices are 32-bit elements; how exact they have to be, the bound alone decides.
A program may use at most 128 MiB of HBM per device.

```python
import math
import jax
import jax.numpy as jnp
import numpy as np
from jax import lax

D = 2048
H = 8
DK = 16
DV = 128
F = 153
SEQ_LEN = 2048
SEQS = 2


def shard_levels(stream_key, shape, cuts, least, high):
    gain, own = 1.0, jax.random.fold_in(stream_key, 6)
    for position, parts in cuts:
        draws = jnp.exp(jax.random.uniform(jax.random.fold_in(own, position), (parts,), jnp.float32, least / len(cuts), high / len(cuts)))
        gain = gain * jnp.repeat(draws, shape[position] // parts).reshape([-1 if axis == position else 1 for axis in range(len(shape))])
    return gain


def bell_draw(stream_key, extent, scale, bound, cuts=(), kind=jnp.bfloat16):
    drawn = scale * jax.random.normal(stream_key, extent, jnp.float32)
    if cuts:
        drawn = drawn * shard_levels(stream_key, extent, cuts, -0.22, 0.18)
    return jnp.clip(drawn, -bound, bound).astype(kind)


def setup_inputs(seed: int = 0) -> dict:
    streams_of = jax.random.split(jax.random.key(seed), 6)
    inputs = bell_draw(streams_of[0], (SEQS, SEQ_LEN, D), 1.0, 6.0, ((0, 2), (1, 16)))
    cotangent = bell_draw(streams_of[1], (SEQS, SEQ_LEN, H * DV), 8.0, 48.0, ((0, 2), (1, 16)))
    w_query = bell_draw(streams_of[2], (D, H * DK), D ** -0.5, 0.125)
    w_key = bell_draw(streams_of[3], (D, H * DK), D ** -0.5, 0.125)
    w_value = bell_draw(streams_of[4], (D, H * DV), D ** -0.5, 0.125)
    return dict(inputs=inputs, cotangent=cotangent, w_query=w_query, w_key=w_key, w_value=w_value)


highest = lax.Precision.HIGHEST

def pair_tables(width):
    rows_idx, cols_idx = np.triu_indices(width)
    eye_table = np.eye(width, dtype=np.float32)
    left_pick = jnp.asarray(eye_table[rows_idx])
    right_pick = jnp.asarray(eye_table[cols_idx])
    pair_coef = jnp.asarray(np.where(rows_idx == cols_idx, 1.0 / math.sqrt(2.0), 1.0).astype(np.float32))
    return (left_pick, right_pick, pair_coef)

def features(scaled, tables):
    left_pick, right_pick, pair_coef = tables
    left_val = jnp.einsum('...d,pd->...p', scaled, left_pick, precision=highest)
    right_val = jnp.einsum('...d,pd->...p', scaled, right_pick, precision=highest)
    leading = jnp.ones(scaled.shape[:-1] + (1,), jnp.float32)
    return jnp.concatenate([leading, scaled, left_val * right_val * pair_coef], -1)

def pull_back(scaled, grad_feat, tables):
    left_pick, right_pick, pair_coef = tables
    width = scaled.shape[-1]
    linear_part = grad_feat[..., 1:1 + width]
    pair_grad = grad_feat[..., 1 + width:] * pair_coef
    left_val = jnp.einsum('...d,pd->...p', scaled, left_pick, precision=highest)
    right_val = jnp.einsum('...d,pd->...p', scaled, right_pick, precision=highest)
    result = linear_part + jnp.einsum('...p,pd->...d', pair_grad * right_val, left_pick, precision=highest)
    return result + jnp.einsum('...p,pd->...d', pair_grad * left_val, right_pick, precision=highest)

def reference(inputs, cotangent, w_query, w_key, w_value):
    tables = pair_tables(DK)
    flat = inputs.reshape(SEQS * SEQ_LEN, D)
    query = jnp.dot(flat, w_query, preferred_element_type=jnp.float32).reshape(SEQS, SEQ_LEN, H, DK)
    keys = jnp.dot(flat, w_key, preferred_element_type=jnp.float32).reshape(SEQS, SEQ_LEN, H, DK)
    values = jnp.dot(flat, w_value, preferred_element_type=jnp.float32).astype(jnp.bfloat16).reshape(SEQS, SEQ_LEN, H, DV)
    feat_q = features(query * 0.5, tables).astype(jnp.bfloat16)
    feat_k = features(keys * 0.5, tables).astype(jnp.bfloat16)
    upstream = cotangent.astype(jnp.float32).reshape(SEQS, SEQ_LEN, H, DV)
    block_len = math.gcd(512, SEQ_LEN)
    nblocks = SEQ_LEN // block_len

    def blocked(array):
        return array.reshape((SEQS, nblocks, block_len) + array.shape[2:]).swapaxes(0, 1)

    def unblocked(array):
        return array.swapaxes(0, 1).reshape((SEQS, SEQ_LEN) + array.shape[3:])
    causal = lax.broadcasted_iota(jnp.int32, (block_len, block_len), 0) >= lax.broadcasted_iota(jnp.int32, (block_len, block_len), 1)

    def scores(fq32, fk32):
        attn = jnp.einsum('bthf,bshf->bhts', fq32, fk32, precision=highest)
        return jnp.where(causal, attn, 0.0)

    def grad_scores(grad_numer, grad_denom, val32):
        inner = jnp.einsum('bthe,bshe->bhts', grad_numer, val32, precision=highest)
        inner = inner + jnp.transpose(grad_denom, (0, 2, 1))[:, :, :, None]
        return jnp.where(causal, inner, 0.0)

    def forward_step(carry, pieces):
        state, norm_state = carry
        fq_blk, fk_blk, val_blk, up_blk = pieces
        fq32 = fq_blk.astype(jnp.float32)
        fk32 = fk_blk.astype(jnp.float32)
        val32 = val_blk.astype(jnp.float32)
        attn = scores(fq32, fk32)
        numerator = jnp.einsum('bhts,bshe->bthe', attn, val32, precision=highest)
        numerator = numerator + jnp.einsum('bthf,bhfe->bthe', fq32, state, precision=highest)
        denominator = jnp.transpose(lax.optimization_barrier(jnp.sum(attn, -1)), (0, 2, 1))
        denominator = denominator + jnp.einsum('bthf,bhf->bth', fq32, norm_state, precision=highest)
        output = numerator / denominator[..., None]
        grad_numer = up_blk / denominator[..., None]
        grad_denom = -lax.optimization_barrier(jnp.sum(up_blk * output, -1)) / denominator
        grad_attn = grad_scores(grad_numer, grad_denom, val32)
        grad_fq = jnp.einsum('bhts,bshf->bthf', grad_attn, fk32, precision=highest)
        grad_fq = grad_fq + jnp.einsum('bhfe,bthe->bthf', state, grad_numer, precision=highest)
        grad_fq = grad_fq + norm_state[:, None, :, :] * grad_denom[..., None]
        state = state + jnp.einsum('bshf,bshe->bhfe', fk32, val32, precision=highest)
        norm_state = norm_state + lax.optimization_barrier(jnp.sum(fk32, 1))
        return ((state, norm_state), (grad_numer, grad_denom, grad_fq))
    start_state = (jnp.zeros((SEQS, H, F, DV), jnp.float32), jnp.zeros((SEQS, H, F), jnp.float32))
    _, (grad_numer, grad_denom, grad_fq) = lax.scan(forward_step, start_state, (blocked(feat_q), blocked(feat_k), blocked(values), blocked(upstream)))

    def reverse_step(carry, pieces):
        back_state, back_norm = carry
        fq_blk, fk_blk, val_blk, numer_blk, denom_blk = pieces
        fq32 = fq_blk.astype(jnp.float32)
        fk32 = fk_blk.astype(jnp.float32)
        val32 = val_blk.astype(jnp.float32)
        attn = scores(fq32, fk32)
        grad_attn = grad_scores(numer_blk, denom_blk, val32)
        grad_val = jnp.einsum('bhts,bthe->bshe', attn, numer_blk, precision=highest)
        grad_val = grad_val + jnp.einsum('bshf,bhfe->bshe', fk32, back_state, precision=highest)
        grad_fk = jnp.einsum('bhts,bthf->bshf', grad_attn, fq32, precision=highest)
        grad_fk = grad_fk + jnp.einsum('bshe,bhfe->bshf', val32, back_state, precision=highest)
        grad_fk = grad_fk + back_norm[:, None, :, :]
        back_state = back_state + jnp.einsum('bthf,bthe->bhfe', fq32, numer_blk, precision=highest)
        back_norm = back_norm + jnp.einsum('bthf,bth->bhf', fq32, denom_blk, precision=highest)
        return ((back_state, back_norm), (grad_val, grad_fk))
    _, (grad_val, grad_fk) = lax.scan(reverse_step, start_state, (blocked(feat_q), blocked(feat_k), blocked(values), grad_numer, grad_denom), reverse=True)
    grad_fq = unblocked(grad_fq)
    grad_fk = unblocked(grad_fk)
    grad_val = unblocked(grad_val)
    grad_query = (pull_back(query * 0.5, grad_fq, tables) * 0.5).astype(jnp.bfloat16).reshape(SEQS * SEQ_LEN, H * DK)
    grad_keys = (pull_back(keys * 0.5, grad_fk, tables) * 0.5).astype(jnp.bfloat16).reshape(SEQS * SEQ_LEN, H * DK)
    grad_values = grad_val.astype(jnp.bfloat16).reshape(SEQS * SEQ_LEN, H * DV)
    grad_in = jnp.dot(grad_query, w_query.T, preferred_element_type=jnp.float32)
    grad_in = grad_in + jnp.dot(grad_keys, w_key.T, preferred_element_type=jnp.float32)
    grad_in = grad_in + jnp.dot(grad_values, w_value.T, preferred_element_type=jnp.float32)
    grad_in = grad_in.astype(jnp.bfloat16).reshape(SEQS, SEQ_LEN, D)
    grad_wq = jnp.dot(flat.T, grad_query, preferred_element_type=jnp.float32)
    grad_wk = jnp.dot(flat.T, grad_keys, preferred_element_type=jnp.float32)
    grad_wv = jnp.dot(flat.T, grad_values, preferred_element_type=jnp.float32)
    return (grad_in, grad_wq, grad_wk, grad_wv)
```

```python
import functools
import math

import jax
import jax.numpy as jnp
import numpy as np
from jax import lax
from jax.experimental import pallas as pl
from jax.experimental.pallas import tpu as pltpu
from jax.sharding import PartitionSpec as P

H = 8
DK = 16
DV = 128
AUX = 16
MESH = pl.DeviceIdType.MESH
BF = jnp.bfloat16
F32 = jnp.float32


def group(kind, outer, inner):
    seq = lax.axis_index("seq")
    core = lax.axis_index("batch")
    high = seq // inner
    low = seq % inner
    if kind == "seq":
        return outer * inner, seq, lambda j: (j, core)
    if kind == "plane":
        return inner * 2, low * 2 + core, lambda j: (high * inner + j // 2, j % 2)
    if kind == "line":
        return outer, high, lambda j: (j * inner + low, core)
    return 2, core, lambda j: (seq, j)


def exchange_kernel(kinds, outer, inner, *refs):
    count = len(kinds)
    ins, outs = refs[:count], refs[count : 2 * count]
    sends, recvs = refs[2 * count : 3 * count], refs[3 * count :]
    groups = [group(kind, outer, inner) for kind in kinds]
    barrier = pltpu.get_barrier_semaphore()
    total = 0
    for size, me, where in groups:
        for k in range(1, size):
            pl.semaphore_signal(
                barrier, inc=1, device_id=where((me + k) % size), device_id_type=MESH
            )
        total += size - 1
    pl.semaphore_wait(barrier, total)
    copies = []
    for (size, me, where), src, dst, send, recv in zip(groups, ins, outs, sends, recvs):
        for k in range(1, size):
            peer = (me + k) % size
            copy = pltpu.make_async_remote_copy(
                src_ref=src.at[peer],
                dst_ref=dst.at[me],
                send_sem=send.at[k],
                recv_sem=recv.at[k],
                device_id=where(peer),
                device_id_type=MESH,
            )
            copy.start()
            copies.append(copy)
    for (size, me, where), src, dst in zip(groups, ins, outs):
        dst[me] = src[me]
    for copy in copies:
        copy.wait()


def exchange(arrays, kinds, outer, inner, number):
    sizes = {"seq": outer * inner, "plane": inner * 2, "line": outer, "pair": 2}
    sems = [pltpu.SemaphoreType.DMA((sizes[k],)) for k in kinds]
    return pl.pallas_call(
        functools.partial(exchange_kernel, kinds, outer, inner),
        out_shape=[jax.ShapeDtypeStruct(a.shape, a.dtype) for a in arrays],
        in_specs=[pl.BlockSpec(memory_space=pltpu.VMEM)] * len(arrays),
        out_specs=[pl.BlockSpec(memory_space=pltpu.VMEM)] * len(arrays),
        scratch_shapes=sems + sems,
        compiler_params=pltpu.CompilerParams(
            collective_id=number, has_side_effects=True, vmem_limit_bytes=60 << 20
        ),
    )(*arrays)


def dot(left, right, dims):
    return lax.dot_general(left, right, ((dims[:1], dims[1:]), ((), ())), preferred_element_type=F32)


def halves(a):
    high = a.astype(BF)
    return high, (a - high.astype(F32)).astype(BF)


def dot2(pair, right, dims):
    return dot(pair[0], right, dims) + dot(pair[1], right, dims)


def dot2r(left, pair, dims):
    return dot(left, pair[0], dims) + dot(left, pair[1], dims)


def dot3(lefts, rights, dims):
    return (
        dot(lefts[0], rights[0], dims)
        + dot(lefts[0], rights[1], dims)
        + dot(lefts[1], rights[0], dims)
    )


def coefs():
    table = np.where(np.eye(DK) > 0, 1.0 / math.sqrt(2.0), 1.0).astype(np.float32)
    table = table * (np.arange(DK)[:, None] <= np.arange(DK)[None, :])
    half = DK // 2
    rows = np.concatenate([table[:half].reshape(-1), table[half:, half:].reshape(-1)])
    return np.ascontiguousarray(np.broadcast_to(rows[:, None], (rows.size, 128)))


def phi(u, coef):
    half = DK // 2
    lanes = u.shape[1]
    pieces = []
    for i in range(DK):
        low = u if i < half else u[half:]
        pieces.append(u[i : i + 1] * low)
    pairs = jnp.concatenate(pieces, 0) * coef
    first = (lax.broadcasted_iota(jnp.int32, (AUX, lanes), 0) == 0).astype(F32)
    return jnp.concatenate([pairs, u, first], 0)


def pull(u, grad, coef):
    half = DK // 2
    pairs = grad[: coef.shape[0]] * coef
    linear = grad[coef.shape[0] : coef.shape[0] + DK]
    rows = lax.broadcasted_iota(jnp.int32, u.shape, 0)
    total = linear
    lower = jnp.zeros_like(u[half:])
    at = 0
    for i in range(DK):
        if i < half:
            piece = pairs[at : at + DK]
            at += DK
            total = total + piece * u[i : i + 1]
            mine = jnp.sum(piece * u, 0, keepdims=True)
        else:
            piece = pairs[at : at + half]
            at += half
            lower = lower + piece * u[i : i + 1]
            mine = jnp.sum(piece * u[half:], 0, keepdims=True)
        total = total + jnp.where(rows == i, mine, 0.0)
    return total + jnp.concatenate([jnp.zeros_like(lower), lower], 0)


def attention_kernel(wide, r_ref, c_ref, o_ref, fq_ref, fk_ref, va_ref, ah, al, gh, gl, nh, nl):
    blocks, _, tokens = r_ref.shape
    length = 2 * tokens
    chunks = blocks // 2
    feats = fq_ref.shape[1]
    coef = jnp.concatenate([c_ref[...]] * (length // 128), 1)
    causal = lax.broadcasted_iota(jnp.int32, (length, length), 0) <= lax.broadcasted_iota(
        jnp.int32, (length, length), 1
    )
    aux_row = lax.broadcasted_iota(jnp.int32, (AUX, length), 0) == 0

    def block(c):
        return jnp.concatenate([r_ref[2 * c], r_ref[2 * c + 1]], 1)

    def store(c, start, rows):
        size = rows.shape[0]
        o_ref[2 * c, start : start + size, :] = rows[:, :tokens]
        o_ref[2 * c + 1, start : start + size, :] = rows[:, tokens:]

    def forward(c, state):
        both = block(c)
        uq = both[:DK] * 0.5
        uk = both[DK : 2 * DK] * 0.5
        val = both[2 * DK : 2 * DK + wide]
        up = both[2 * DK + wide :]
        fq = phi(uq, coef).astype(BF)
        fk = phi(uk, coef).astype(BF)
        va = jnp.concatenate([val, aux_row.astype(F32)], 0).astype(BF)
        fq_ref[c] = fq
        fk_ref[c] = fk
        va_ref[c] = va
        attn = halves(jnp.where(causal, dot(fk, fq, (0, 0)), 0.0))
        ah[c] = attn[0]
        al[c] = attn[1]
        held = halves(state)
        top = dot2r(va, attn, (1, 0)) + dot2(held, fq, (1, 0))
        scale = 1.0 / top[wide : wide + 1]
        numer = up * scale
        denom = -jnp.sum(numer * top[:wide], 0, keepdims=True) * scale
        gn = halves(jnp.concatenate([numer, jnp.where(aux_row, denom, 0.0)], 0))
        nh[c] = gn[0]
        nl[c] = gn[1]
        ga = halves(jnp.where(causal, dot2r(va, gn, (0, 0)), 0.0))
        gh[c] = ga[0]
        gl[c] = ga[1]
        gfq = dot2r(fk, ga, (1, 0)) + dot3(held, gn, (0, 0))
        store(c, 0, pull(uq, gfq, coef) * 0.5)
        return state + dot(va, fk, (1, 1))

    zero = jnp.zeros((wide + AUX, feats), F32)
    lax.fori_loop(0, chunks, forward, zero)

    def backward(step, state):
        c = chunks - 1 - step
        uk = block(c)[DK : 2 * DK] * 0.5
        fq, fk, va = fq_ref[c], fk_ref[c], va_ref[c]
        attn = (ah[c], al[c])
        ga = (gh[c], gl[c])
        gn = (nh[c], nl[c])
        held = halves(state)
        gv = dot3(gn, attn, (1, 1)) + dot2(held, fk, (1, 0))
        store(c, 2 * DK, gv[:wide])
        gfk = dot2r(fq, ga, (1, 1)) + dot2(held, va, (0, 0))
        store(c, DK, pull(uk, gfk, coef) * 0.5)
        return state + dot2(gn, fq, (1, 1))

    lax.fori_loop(0, chunks, backward, zero)


def attention(received, wide):
    blocks, _, tokens = received.shape
    coef = coefs()
    feats = coef.shape[0] + DK + AUX
    chunks, length = blocks // 2, 2 * tokens
    square = pltpu.VMEM((chunks, length, length), BF)
    grads = pltpu.VMEM((chunks, wide + AUX, length), BF)
    feat = pltpu.VMEM((chunks, feats, length), BF)
    return pl.pallas_call(
        functools.partial(attention_kernel, wide),
        out_shape=jax.ShapeDtypeStruct((blocks, 2 * DK + wide, tokens), F32),
        in_specs=[pl.BlockSpec(memory_space=pltpu.VMEM)] * 2,
        out_specs=pl.BlockSpec(memory_space=pltpu.VMEM),
        scratch_shapes=[feat, feat, grads, square, square, square, square, grads, grads],
        compiler_params=pltpu.CompilerParams(vmem_limit_bytes=60 << 20),
    )(received, jnp.asarray(coef))


def body(inputs, cotangent, w_query, w_key, w_value):
    seqs = lax.axis_size("seq")
    outer = 4 if seqs % 4 == 0 else 1
    inner = seqs // outer
    split = seqs // H
    wide = DV // split
    tokens = inputs[0]
    length, width = tokens.shape
    weights = jnp.concatenate([w_query, w_key, w_value], 1)
    cols = weights.shape[1]
    qk = H * DK
    proj = lax.dot_general(weights, tokens, (((0,), (1,)), ((), ())), preferred_element_type=F32)
    heads = proj[: 2 * qk].reshape(2, H, 1, DK, length)
    heads = jnp.broadcast_to(heads, (2, H, split, DK, length)).reshape(2, seqs, DK, length)
    values = proj[2 * qk :].astype(BF).astype(F32).reshape(seqs, wide, length)
    upstream = cotangent[0].astype(F32).T.reshape(seqs, wide, length)
    sent = jnp.concatenate([heads[0], heads[1], values, upstream], 1)
    rows = width // seqs
    staged = tokens.astype(F32).reshape(length, outer, inner, rows).transpose(2, 0, 1, 3)
    staged = staged.reshape(inner, 1, length, outer * rows)
    staged = jnp.broadcast_to(staged, (inner, 2, length, outer * rows))
    staged = staged.reshape(inner * 2, length, outer * rows)
    received, group_in = exchange([sent, staged], ["seq", "plane"], outer, inner, 0)
    back = attention(received, wide)
    (grads,) = exchange([back], ["seq"], outer, inner, 1)
    small = grads[:, : 2 * DK].reshape(H, split, 2, DK, length).sum(1)
    small = small.transpose(1, 0, 2, 3).reshape(2 * qk, length)
    joined = jnp.concatenate([small, grads[:, 2 * DK :].reshape(H * DV, length)], 0).astype(BF)
    grad_in = lax.dot_general(
        joined, weights, (((0,), (1,)), ((), ())), preferred_element_type=F32
    ).astype(BF)[None]
    part = joined.astype(F32).reshape(1, 2, cols // 2, length)
    part = jnp.broadcast_to(part, (inner, 2, cols // 2, length)).reshape(
        inner * 2, cols // 2, length
    )
    (group_grad,) = exchange([part], ["plane"], outer, inner, 2)
    partial = jnp.einsum(
        "gtr,gct->rc", group_in.astype(BF), group_grad.astype(BF), preferred_element_type=F32
    )
    (lined,) = exchange([partial.reshape(outer, rows, cols // 2)], ["line"], outer, inner, 3)
    summed = lined.sum(0).reshape(2, rows // 2, cols // 2)
    (paired,) = exchange([summed], ["pair"], outer, inner, 4)
    reduced = paired.transpose(1, 0, 2).reshape(rows // 2, cols)
    return (grad_in, reduced[:, :qk], reduced[:, qk : 2 * qk], reduced[:, 2 * qk :])


def solution(mesh):
    in_specs = (P("batch", "seq", None), P("batch", "seq", None), P(), P(), P())
    out_specs = (
        P("batch", "seq", None),
        P(("seq", "batch"), None),
        P(("seq", "batch"), None),
        P(("seq", "batch"), None),
    )
    return jax.shard_map(body, mesh=mesh, in_specs=in_specs, out_specs=out_specs, check_vma=False)
```

```python
import functools
import math

import jax
import jax.numpy as jnp
import numpy as np
from jax import lax
from jax.experimental import pallas as pl
from jax.experimental.pallas import tpu as pltpu
from jax.sharding import PartitionSpec as P

H = 8
DK = 16
DV = 128
AUX = 16
MESH = pl.DeviceIdType.MESH
BF = jnp.bfloat16
F32 = jnp.float32


def group(kind, outer, inner):
    seq = lax.axis_index("seq")
    core = lax.axis_index("batch")
    high = seq // inner
    low = seq % inner
    if kind == "seq":
        return outer * inner, seq, lambda j: (j, core)
    if kind == "plane":
        return inner * 2, low * 2 + core, lambda j: (high * inner + j // 2, j % 2)
    if kind == "line":
        return outer, high, lambda j: (j * inner + low, core)
    if kind == "chips":
        return inner, low, lambda j: (high * inner + j, core)
    return 2, core, lambda j: (seq, j)


def greet(groups):
    barrier = pltpu.get_barrier_semaphore()
    total = 0
    for size, me, where in groups:
        for k in range(1, size):
            pl.semaphore_signal(
                barrier, inc=1, device_id=where((me + k) % size), device_id_type=MESH
            )
        total += size - 1
    pl.semaphore_wait(barrier, total)


def push(src, dst, send, recv, device):
    copy = pltpu.make_async_remote_copy(
        src_ref=src,
        dst_ref=dst,
        send_sem=send,
        recv_sem=recv,
        device_id=device,
        device_id_type=MESH,
    )
    copy.start()
    return copy


def exchange_kernel(outer, inner, src, dst, send, recv):
    size, me, where = group("seq", outer, inner)
    greet([(size, me, where)])
    copies = []
    for k in range(1, size):
        peer = (me + k) % size
        copies.append(push(src.at[peer], dst.at[me], send.at[k], recv.at[k], where(peer)))
    dst[me] = src[me]
    for copy in copies:
        copy.wait()


VMEM = pl.BlockSpec(memory_space=pltpu.VMEM)
HBM = pl.BlockSpec(memory_space=pl.ANY)


def sems(*sizes):
    return pltpu.SemaphoreType.DMA(sizes)


def params(number):
    return pltpu.CompilerParams(
        collective_id=number, has_side_effects=True, vmem_limit_bytes=60 << 20
    )


def exchange(array, outer, inner):
    return pl.pallas_call(
        functools.partial(exchange_kernel, outer, inner),
        out_shape=jax.ShapeDtypeStruct(array.shape, array.dtype),
        in_specs=[VMEM],
        out_specs=VMEM,
        scratch_shapes=[sems(outer * inner), sems(outer * inner)],
        compiler_params=params(1),
    )(array)


def dot(left, right, dims):
    return lax.dot_general(left, right, ((dims[:1], dims[1:]), ((), ())), preferred_element_type=F32)


def halves(a):
    high = a.astype(BF)
    return high, (a - high.astype(F32)).astype(BF)


def dot2(pair, right, dims):
    return dot(pair[0], right, dims) + dot(pair[1], right, dims)


def dot2r(left, pair, dims):
    return dot(left, pair[0], dims) + dot(left, pair[1], dims)


def dot3(lefts, rights, dims):
    return (
        dot(lefts[0], rights[0], dims)
        + dot(lefts[0], rights[1], dims)
        + dot(lefts[1], rights[0], dims)
    )


def coefs():
    table = np.where(np.eye(DK) > 0, 1.0 / math.sqrt(2.0), 1.0).astype(np.float32)
    table = table * (np.arange(DK)[:, None] <= np.arange(DK)[None, :])
    half = DK // 2
    rows = np.concatenate([table[:half].reshape(-1), table[half:, half:].reshape(-1)])
    return np.ascontiguousarray(np.broadcast_to(rows[:, None], (rows.size, 128)))


def phi(u, coef):
    half = DK // 2
    lanes = u.shape[1]
    pieces = []
    for i in range(DK):
        low = u if i < half else u[half:]
        pieces.append(u[i : i + 1] * low)
    pairs = jnp.concatenate(pieces, 0) * coef
    first = (lax.broadcasted_iota(jnp.int32, (AUX, lanes), 0) == 0).astype(F32)
    return jnp.concatenate([pairs, u, first], 0)


def pull(u, grad, coef):
    half = DK // 2
    pairs = grad[: coef.shape[0]] * coef
    linear = grad[coef.shape[0] : coef.shape[0] + DK]
    rows = lax.broadcasted_iota(jnp.int32, u.shape, 0)
    total = linear
    lower = jnp.zeros_like(u[half:])
    at = 0
    for i in range(DK):
        if i < half:
            piece = pairs[at : at + DK]
            at += DK
            total = total + piece * u[i : i + 1]
            mine = jnp.sum(piece * u, 0, keepdims=True)
        else:
            piece = pairs[at : at + half]
            at += half
            lower = lower + piece * u[i : i + 1]
            mine = jnp.sum(piece * u[half:], 0, keepdims=True)
        total = total + jnp.where(rows == i, mine, 0.0)
    return total + jnp.concatenate([jnp.zeros_like(lower), lower], 0)


def attention_kernel(wide, r_ref, c_ref, o_ref, fq_ref, fk_ref, va_ref, ah, al, gh, gl, nh, nl):
    blocks, _, tokens = r_ref.shape
    length = 2 * tokens
    chunks = blocks // 2
    feats = fq_ref.shape[1]
    coef = jnp.concatenate([c_ref[...]] * (length // 128), 1)
    causal = lax.broadcasted_iota(jnp.int32, (length, length), 0) <= lax.broadcasted_iota(
        jnp.int32, (length, length), 1
    )
    aux_row = lax.broadcasted_iota(jnp.int32, (AUX, length), 0) == 0

    def block(c):
        return jnp.concatenate([r_ref[2 * c], r_ref[2 * c + 1]], 1)

    def store(c, start, rows):
        size = rows.shape[0]
        o_ref[2 * c, start : start + size, :] = rows[:, :tokens]
        o_ref[2 * c + 1, start : start + size, :] = rows[:, tokens:]

    def forward(c, state):
        both = block(c)
        uq = both[:DK] * 0.5
        uk = both[DK : 2 * DK] * 0.5
        val = both[2 * DK : 2 * DK + wide]
        up = both[2 * DK + wide :]
        fq = phi(uq, coef).astype(BF)
        fk = phi(uk, coef).astype(BF)
        va = jnp.concatenate([val, aux_row.astype(F32)], 0).astype(BF)
        fq_ref[c] = fq
        fk_ref[c] = fk
        va_ref[c] = va
        attn = halves(jnp.where(causal, dot(fk, fq, (0, 0)), 0.0))
        ah[c] = attn[0]
        al[c] = attn[1]
        held = halves(state)
        top = dot2r(va, attn, (1, 0)) + dot2(held, fq, (1, 0))
        scale = 1.0 / top[wide : wide + 1]
        numer = up * scale
        denom = -jnp.sum(numer * top[:wide], 0, keepdims=True) * scale
        gn = halves(jnp.concatenate([numer, jnp.where(aux_row, denom, 0.0)], 0))
        nh[c] = gn[0]
        nl[c] = gn[1]
        ga = halves(jnp.where(causal, dot2r(va, gn, (0, 0)), 0.0))
        gh[c] = ga[0]
        gl[c] = ga[1]
        gfq = dot2r(fk, ga, (1, 0)) + dot3(held, gn, (0, 0))
        store(c, 0, pull(uq, gfq, coef) * 0.5)
        return state + dot(va, fk, (1, 1))

    zero = jnp.zeros((wide + AUX, feats), F32)
    lax.fori_loop(0, chunks, forward, zero)

    def backward(step, state):
        c = chunks - 1 - step
        uk = block(c)[DK : 2 * DK] * 0.5
        fq, fk, va = fq_ref[c], fk_ref[c], va_ref[c]
        attn = (ah[c], al[c])
        ga = (gh[c], gl[c])
        gn = (nh[c], nl[c])
        held = halves(state)
        gv = dot3(gn, attn, (1, 1)) + dot2(held, fk, (1, 0))
        store(c, 2 * DK, gv[:wide])
        gfk = dot2r(fq, ga, (1, 1)) + dot2(held, va, (0, 0))
        store(c, DK, pull(uk, gfk, coef) * 0.5)
        return state + dot2(gn, fq, (1, 1))

    lax.fori_loop(0, chunks, backward, zero)


def attention(received, wide):
    blocks, _, tokens = received.shape
    coef = coefs()
    feats = coef.shape[0] + DK + AUX
    chunks, length = blocks // 2, 2 * tokens
    square = pltpu.VMEM((chunks, length, length), BF)
    grads = pltpu.VMEM((chunks, wide + AUX, length), BF)
    feat = pltpu.VMEM((chunks, feats, length), BF)
    return pl.pallas_call(
        functools.partial(attention_kernel, wide),
        out_shape=jax.ShapeDtypeStruct((blocks, 2 * DK + wide, tokens), F32),
        in_specs=[pl.BlockSpec(memory_space=pltpu.VMEM)] * 2,
        out_specs=pl.BlockSpec(memory_space=pltpu.VMEM),
        scratch_shapes=[feat, feat, grads, square, square, square, square, grads, grads],
        compiler_params=pltpu.CompilerParams(vmem_limit_bytes=60 << 20),
    )(received, jnp.asarray(coef))


def front_kernel(
    outer, inner, x_ref, up_ref, in_ref, wq_hbm, wk_hbm, wv_hbm, out_ref, got_ref,
    wq_ref, wk_ref, wv_ref, own_ref, load, send_u, recv_u, send_i, recv_i, send_p, recv_p,
):
    loads = []
    for n, (src, dst) in enumerate(((wq_hbm, wq_ref), (wk_hbm, wk_ref), (wv_hbm, wv_ref))):
        copy = pltpu.make_async_copy(src, dst, load.at[n])
        copy.start()
        loads.append(copy)
    size, me, where = group("seq", outer, inner)
    chips, low, chip = group("chips", outer, inner)
    greet([(size, me, where), (chips, low, chip)])
    split = size // H
    wide = DV // split
    cut = 2 * DK + wide
    copies = []
    for k in range(1, size):
        peer = (me + k) % size
        dst = out_ref.at[me, pl.ds(cut, wide)]
        copies.append(push(up_ref.at[peer], dst, send_u.at[k], recv_u.at[k], where(peer)))
    for k in range(1, chips):
        peer = (low + k) % chips
        copies.append(
            push(in_ref.at[peer], got_ref.at[low], send_i.at[k], recv_i.at[k], chip(peer))
        )
    x = x_ref[...]
    for n, (w_ref, copy) in enumerate(zip((wq_ref, wk_ref), loads)):
        copy.wait()
        flat = dot(x, w_ref[...], (1, 0)).T
        for s in range(size):
            at = (s // split) * DK
            own_ref[s, n * DK : (n + 1) * DK, :] = flat[at : at + DK]
    loads[2].wait()
    for s in range(0, size, DV // wide):
        at = s * wide
        flat = dot(x, wv_ref[:, at : at + DV], (1, 0)).astype(BF).astype(F32).T
        for n in range(DV // wide):
            own_ref[s + n, 2 * DK :, :] = flat[n * wide : (n + 1) * wide]
    for k in range(1, size):
        peer = (me + k) % size
        dst = out_ref.at[me, pl.ds(0, cut)]
        copies.append(push(own_ref.at[peer], dst, send_p.at[k], recv_p.at[k], where(peer)))
    out_ref[me, :cut, :] = own_ref[me]
    out_ref[me, cut:, :] = up_ref[me]
    got_ref[low] = in_ref[low]
    for copy in copies:
        copy.wait()


def front(tokens, upstream, staged, weights, outer, inner):
    seqs, wide, length = upstream.shape
    cut = 2 * DK + wide
    w_scratch = [pltpu.VMEM(w.shape, w.dtype) for w in weights]
    pairs = [sems(seqs), sems(seqs), sems(inner), sems(inner), sems(seqs), sems(seqs)]
    return pl.pallas_call(
        functools.partial(front_kernel, outer, inner),
        out_shape=[
            jax.ShapeDtypeStruct((seqs, cut + wide, length), F32),
            jax.ShapeDtypeStruct(staged.shape, F32),
        ],
        in_specs=[VMEM] * 3 + [HBM] * 3,
        out_specs=[VMEM] * 2,
        scratch_shapes=w_scratch + [pltpu.VMEM((seqs, cut, length), F32), sems(3)] + pairs,
        compiler_params=params(0),
    )(tokens, upstream, staged, *weights)


def tail_kernel(
    outer, inner, pieces, g_ref, in_ref, wq_hbm, wk_hbm, wv_hbm, gi_ref, o_ref,
    wq_ref, wk_ref, wv_ref, jt_ref, jb_ref, gj_ref, pg_ref, xb_ref, ls_ref, lr_ref, fs_ref, os_ref,
    load, send_x, recv_x, send_j, recv_j, send_l, recv_l, send_o, recv_o,
):
    loads = []
    for n, (src, dst) in enumerate(((wq_hbm, wq_ref), (wk_hbm, wk_ref), (wv_hbm, wv_ref))):
        copy = pltpu.make_async_copy(src, dst, load.at[n])
        copy.start()
        loads.append(copy)
    plane, mine, where = group("plane", outer, inner)
    lines, high, along = group("line", outer, inner)
    _, core, sibling = group("pair", outer, inner)
    greet([(plane, mine, where), (lines, high, along), (2, core, sibling)])
    other = 1 - core
    pending = [push(in_ref, pg_ref, send_x.at[0], recv_x.at[0], sibling(other))]
    seqs = outer * inner
    split = seqs // H
    wide = DV // split
    blocks = []
    for n in range(2):
        rows = []
        for h in range(H):
            total = g_ref[h * split, n * DK : (n + 1) * DK, :]
            for s in range(1, split):
                total = total + g_ref[h * split + s, n * DK : (n + 1) * DK, :]
            rows.append(total)
        blocks.append(jnp.concatenate(rows, 0))
    for h in range(H):
        blocks.append(
            jnp.concatenate([g_ref[h * split + s, 2 * DK :, :] for s in range(split)], 0)
        )
    for i in range(pieces):
        for half in range(2):
            jb_ref[half, i] = blocks[half * pieces + i].astype(BF).astype(F32)
    gathers = []
    for i in range(pieces):
        row = []
        for k in range(1, plane):
            peer = (mine + k) % plane
            src = jb_ref.at[peer % 2, i]
            row.append(
                push(src, gj_ref.at[i, mine], send_j.at[i, k], recv_j.at[i, k], where(peer))
            )
        gathers.append(row)
    for n, block in enumerate(blocks):
        jt_ref[:, n * DV : (n + 1) * DV] = block.T.astype(BF)
    for i in range(pieces):
        gj_ref[i, mine] = jb_ref[core, i]
    for j in range(inner):
        xb_ref[2 * j + core] = in_ref[j].astype(BF)
    for copy in loads:
        copy.wait()
    depth = gi_ref.shape[1] // pieces // 256 * 256
    starts = [i * depth for i in range(pieces)] + [gi_ref.shape[1]]
    pending[0].wait()
    for j in range(inner):
        xb_ref[2 * j + other] = pg_ref[j].astype(BF)
    tokens = plane * in_ref.shape[1]
    rows = in_ref.shape[2] // lines
    reduces = []
    for i in range(pieces):
        cut = slice(starts[i], starts[i + 1])
        total = dot(jt_ref[:, :DV], wq_ref[cut, :], (1, 1))
        total = total + dot(jt_ref[:, DV : 2 * DV], wk_ref[cut, :], (1, 1))
        total = total + dot(jt_ref[:, 2 * DV :], wv_ref[cut, :], (1, 1))
        gi_ref[:, cut] = total.astype(BF)
        for copy in gathers[i]:
            copy.wait_recv()
        grads = jnp.concatenate([gj_ref[i, j].astype(BF) for j in range(plane)], 1)
        part = dot(grads, xb_ref[...].reshape(tokens, in_ref.shape[2]), (1, 0))
        for z in range(lines):
            ls_ref[i, z] = part[:, z * rows : (z + 1) * rows]
        row = []
        for k in range(1, lines):
            peer = (high + k) % lines
            row.append(
                push(ls_ref.at[i, peer], lr_ref.at[i, k], send_l.at[i, k], recv_l.at[i, k], along(peer))
            )
        reduces.append(row)
    lasts = []
    keep = rows // 2
    for i in range(pieces):
        total = ls_ref[i, high]
        for k, copy in enumerate(reduces[i]):
            copy.wait_recv()
            total = total + lr_ref[i, k + 1]
        fs_ref[i] = total.T
        src = fs_ref.at[i, pl.ds(pl.multiple_of(other * keep, keep), keep)]
        lasts.append(push(src, os_ref.at[i], send_o.at[i], recv_o.at[i], sibling(other)))
        o_ref[core * pieces + i] = fs_ref[i, pl.ds(pl.multiple_of(core * keep, keep), keep), :]
    for i, copy in enumerate(lasts):
        copy.wait_recv()
        o_ref[other * pieces + i] = os_ref[i]
    for row in gathers + reduces + [lasts]:
        for copy in row:
            copy.wait_send()


def tail(grads, inside, weights, outer, inner):
    seqs, _, length = grads.shape
    width = weights[0].shape[0]
    pieces = sum(w.shape[1] for w in weights) // (2 * DV)
    rows = width // seqs
    plane = 2 * inner
    vm = lambda *shape: pltpu.VMEM(shape, F32)
    scratch = [pltpu.VMEM(w.shape, w.dtype) for w in weights] + [
        pltpu.VMEM((length, 2 * pieces * DV), BF),
        vm(2, pieces, DV, length),
        vm(pieces, plane, DV, length),
        vm(inner, length, outer * rows),
        pltpu.VMEM((plane, length, outer * rows), BF),
        vm(pieces, outer, DV, rows),
        vm(pieces, outer, DV, rows),
        vm(pieces, rows, DV),
        vm(pieces, rows // 2, DV),
        sems(3), sems(1), sems(1),
        sems(pieces, plane), sems(pieces, plane),
        sems(pieces, outer), sems(pieces, outer),
        sems(pieces), sems(pieces),
    ]
    return pl.pallas_call(
        functools.partial(tail_kernel, outer, inner, pieces),
        out_shape=[
            jax.ShapeDtypeStruct((length, width), BF),
            jax.ShapeDtypeStruct((2 * pieces, rows // 2, DV), F32),
        ],
        in_specs=[VMEM] * 2 + [HBM] * 3,
        out_specs=[VMEM] * 2,
        scratch_shapes=scratch,
        compiler_params=params(2),
    )(grads, inside, *weights)


def body(inputs, cotangent, w_query, w_key, w_value):
    seqs = lax.axis_size("seq")
    outer = 4 if seqs % 4 == 0 else 1
    inner = seqs // outer
    wide = DV * H // seqs
    tokens = inputs[0]
    length, width = tokens.shape
    weights = (w_query, w_key, w_value)
    upstream = cotangent[0].astype(F32).T.reshape(seqs, wide, length)
    rows = width // seqs
    staged = tokens.astype(F32).reshape(length, outer, inner, rows).transpose(2, 0, 1, 3)
    staged = staged.reshape(inner, length, outer * rows)
    received, inside = front(tokens, upstream, staged, weights, outer, inner)
    back = attention(received, wide)
    grads = exchange(back, outer, inner)
    grad_in, blocks = tail(grads, inside, weights, outer, inner)
    grad_wv = blocks[2:].transpose(1, 0, 2).reshape(rows // 2, H * DV)
    return (grad_in[None], blocks[0], blocks[1], grad_wv)


def solution(mesh):
    in_specs = (P("batch", "seq", None), P("batch", "seq", None), P(), P(), P())
    out_specs = (
        P("batch", "seq", None),
        P(("seq", "batch"), None),
        P(("seq", "batch"), None),
        P(("seq", "batch"), None),
    )
    return jax.shard_map(body, mesh=mesh, in_specs=in_specs, out_specs=out_specs, check_vma=False)
```

```python
import functools
import math

import jax
import jax.numpy as jnp
import numpy as np
from jax import lax
from jax.experimental import pallas as pl
from jax.experimental.pallas import tpu as pltpu
from jax.sharding import PartitionSpec as P

H = 8
DK = 16
DV = 128
AUX = 16
MESH = pl.DeviceIdType.MESH
BF = jnp.bfloat16
F32 = jnp.float32


def group(kind, outer, inner):
    seq = lax.axis_index("seq")
    core = lax.axis_index("batch")
    high = seq // inner
    low = seq % inner
    if kind == "seq":
        return outer * inner, seq, lambda j: (j, core)
    if kind == "plane":
        return inner * 2, low * 2 + core, lambda j: (high * inner + j // 2, j % 2)
    if kind == "line":
        return outer, high, lambda j: (j * inner + low, core)
    if kind == "chips":
        return inner, low, lambda j: (high * inner + j, core)
    return 2, core, lambda j: (seq, j)


def greet(groups):
    barrier = pltpu.get_barrier_semaphore()
    total = 0
    for size, me, where in groups:
        for k in range(1, size):
            pl.semaphore_signal(
                barrier, inc=1, device_id=where((me + k) % size), device_id_type=MESH
            )
        total += size - 1
    pl.semaphore_wait(barrier, total)


def push(src, dst, send, recv, device):
    copy = pltpu.make_async_remote_copy(
        src_ref=src,
        dst_ref=dst,
        send_sem=send,
        recv_sem=recv,
        device_id=device,
        device_id_type=MESH,
    )
    copy.start()
    return copy


VMEM = pl.BlockSpec(memory_space=pltpu.VMEM)
HBM = pl.BlockSpec(memory_space=pl.ANY)


def sems(*sizes):
    return pltpu.SemaphoreType.DMA(sizes)


def params(number):
    return pltpu.CompilerParams(
        collective_id=number, has_side_effects=True, vmem_limit_bytes=60 << 20
    )


def dot(left, right, dims):
    return lax.dot_general(left, right, ((dims[:1], dims[1:]), ((), ())), preferred_element_type=F32)


def halves(a):
    high = a.astype(BF)
    return high, (a - high.astype(F32)).astype(BF)


def dot2(pair, right, dims):
    return dot(pair[0], right, dims) + dot(pair[1], right, dims)


def dot2r(left, pair, dims):
    return dot(left, pair[0], dims) + dot(left, pair[1], dims)


def dot3(lefts, rights, dims):
    return (
        dot(lefts[0], rights[0], dims)
        + dot(lefts[0], rights[1], dims)
        + dot(lefts[1], rights[0], dims)
    )


def coefs():
    table = np.where(np.eye(DK) > 0, 1.0 / math.sqrt(2.0), 1.0).astype(np.float32)
    table = table * (np.arange(DK)[:, None] <= np.arange(DK)[None, :])
    half = DK // 2
    rows = np.concatenate([table[:half].reshape(-1), table[half:, half:].reshape(-1)])
    return np.ascontiguousarray(np.broadcast_to(rows[:, None], (rows.size, 128)))


def phi(u, coef):
    half = DK // 2
    lanes = u.shape[1]
    pieces = []
    for i in range(DK):
        low = u if i < half else u[half:]
        pieces.append(u[i : i + 1] * low)
    pairs = jnp.concatenate(pieces, 0) * coef
    first = (lax.broadcasted_iota(jnp.int32, (AUX, lanes), 0) == 0).astype(F32)
    return jnp.concatenate([pairs, u, first], 0)


def pull(u, grad, coef):
    half = DK // 2
    pairs = grad[: coef.shape[0]] * coef
    linear = grad[coef.shape[0] : coef.shape[0] + DK]
    rows = lax.broadcasted_iota(jnp.int32, u.shape, 0)
    total = linear
    lower = jnp.zeros_like(u[half:])
    at = 0
    for i in range(DK):
        if i < half:
            piece = pairs[at : at + DK]
            at += DK
            total = total + piece * u[i : i + 1]
            mine = jnp.sum(piece * u, 0, keepdims=True)
        else:
            piece = pairs[at : at + half]
            at += half
            lower = lower + piece * u[i : i + 1]
            mine = jnp.sum(piece * u[half:], 0, keepdims=True)
        total = total + jnp.where(rows == i, mine, 0.0)
    return total + jnp.concatenate([jnp.zeros_like(lower), lower], 0)


def attention_kernel(
    wide, outer, inner, r_ref, c_ref, x_ref, got_ref, xb_ref,
    o_ref, fq_ref, fk_ref, va_ref, ah, al, gh, gl, nh, nl, st_ref, gi_ref, pg_ref,
    send_i, recv_i, send_x, recv_x, send_r, recv_r,
):
    blocks, _, tokens = r_ref.shape
    size, me, where = group("seq", outer, inner)
    chips, low, chip = group("chips", outer, inner)
    _, core, sibling = group("pair", outer, inner)
    rows = st_ref.shape[2] // outer
    for j in range(inner):
        for z in range(outer):
            at = (z * inner + j) * rows
            st_ref[j, :, z * rows : (z + 1) * rows] = x_ref[:, at : at + rows].astype(F32)
    greet([(size, me, where), (chips, low, chip), (2, core, sibling)])
    inside = []
    for k in range(1, chips):
        peer = (low + k) % chips
        inside.append(
            push(st_ref.at[peer], gi_ref.at[low], send_i.at[k], recv_i.at[k], chip(peer))
        )
    gi_ref[low] = st_ref[low]
    length = 2 * tokens
    chunks = blocks // 2
    feats = fq_ref.shape[1]
    coef = jnp.concatenate([c_ref[...]] * (length // 128), 1)
    causal = lax.broadcasted_iota(jnp.int32, (length, length), 0) <= lax.broadcasted_iota(
        jnp.int32, (length, length), 1
    )
    aux_row = lax.broadcasted_iota(jnp.int32, (AUX, length), 0) == 0

    def block(c):
        return jnp.concatenate([r_ref[2 * c], r_ref[2 * c + 1]], 1)

    def store(c, start, rows):
        size = rows.shape[0]
        o_ref[2 * c, start : start + size, :] = rows[:, :tokens]
        o_ref[2 * c + 1, start : start + size, :] = rows[:, tokens:]

    def forward(c, state):
        both = block(c)
        uq = both[:DK] * 0.5
        uk = both[DK : 2 * DK] * 0.5
        val = both[2 * DK : 2 * DK + wide]
        up = both[2 * DK + wide :]
        fq = phi(uq, coef).astype(BF)
        fk = phi(uk, coef).astype(BF)
        va = jnp.concatenate([val, aux_row.astype(F32)], 0).astype(BF)
        fq_ref[c] = fq
        fk_ref[c] = fk
        va_ref[c] = va
        attn = halves(jnp.where(causal, dot(fk, fq, (0, 0)), 0.0))
        ah[c] = attn[0]
        al[c] = attn[1]
        held = halves(state)
        top = dot2r(va, attn, (1, 0)) + dot2(held, fq, (1, 0))
        scale = 1.0 / top[wide : wide + 1]
        numer = up * scale
        denom = -jnp.sum(numer * top[:wide], 0, keepdims=True) * scale
        gn = halves(jnp.concatenate([numer, jnp.where(aux_row, denom, 0.0)], 0))
        nh[c] = gn[0]
        nl[c] = gn[1]
        ga = halves(jnp.where(causal, dot2r(va, gn, (0, 0)), 0.0))
        gh[c] = ga[0]
        gl[c] = ga[1]
        gfq = dot2r(fk, ga, (1, 0)) + dot3(held, gn, (0, 0))
        store(c, 0, pull(uq, gfq, coef) * 0.5)
        return state + dot(va, fk, (1, 1))

    zero = jnp.zeros((wide + AUX, feats), F32)
    lax.fori_loop(0, chunks, forward, zero)

    def backward(step, state):
        c = chunks - 1 - step
        uk = block(c)[DK : 2 * DK] * 0.5
        fq, fk, va = fq_ref[c], fk_ref[c], va_ref[c]
        attn = (ah[c], al[c])
        ga = (gh[c], gl[c])
        gn = (nh[c], nl[c])
        held = halves(state)
        gv = dot3(gn, attn, (1, 1)) + dot2(held, fk, (1, 0))
        store(c, 2 * DK, gv[:wide])
        gfk = dot2r(fq, ga, (1, 1)) + dot2(held, va, (0, 0))
        store(c, DK, pull(uk, gfk, coef) * 0.5)
        for t in range(2):
            peer = 2 * c + t

            @pl.when(peer != me)
            def _():
                push(o_ref.at[peer], got_ref.at[me], send_r.at[peer], recv_r.at[me], where(peer))

        return state + dot2(gn, fq, (1, 1))

    lax.fori_loop(0, chunks, backward, zero)
    got_ref[me] = o_ref[me]
    for copy in inside:
        copy.wait()
    pair = push(gi_ref, pg_ref, send_x.at[0], recv_x.at[0], sibling(1 - core))
    for j in range(inner):
        xb_ref[2 * j + core] = gi_ref[j].astype(BF)
    pair.wait()
    for j in range(inner):
        xb_ref[2 * j + 1 - core] = pg_ref[j].astype(BF)
    for k in range(1, size):
        peer = (me + k) % size
        pltpu.make_async_remote_copy(
            src_ref=o_ref.at[peer],
            dst_ref=got_ref.at[peer],
            send_sem=send_r.at[peer],
            recv_sem=recv_r.at[peer],
            device_id=where(peer),
            device_id_type=MESH,
        ).wait()


def attention(received, tokens_in, wide, outer, inner):
    blocks, _, tokens = received.shape
    coef = coefs()
    feats = coef.shape[0] + DK + AUX
    chunks, length = blocks // 2, 2 * tokens
    width = tokens_in.shape[1] // inner
    square = pltpu.VMEM((chunks, length, length), BF)
    grads = pltpu.VMEM((chunks, wide + AUX, length), BF)
    feat = pltpu.VMEM((chunks, feats, length), BF)
    result = (blocks, 2 * DK + wide, tokens)
    group_in = pltpu.VMEM((inner, tokens, width), F32)
    scratch = [pltpu.VMEM(result, F32), feat, feat, grads, square, square, square, square]
    scratch += [grads, grads, group_in, group_in, group_in]
    scratch += [sems(inner)] * 2 + [sems(1)] * 2 + [sems(blocks)] * 2
    return pl.pallas_call(
        functools.partial(attention_kernel, wide, outer, inner),
        out_shape=[
            jax.ShapeDtypeStruct(result, F32),
            jax.ShapeDtypeStruct((2 * inner, tokens, width), BF),
        ],
        in_specs=[VMEM] * 3,
        out_specs=[VMEM] * 2,
        scratch_shapes=scratch,
        compiler_params=params(1),
    )(received, jnp.asarray(coef), tokens_in)


def front_kernel(
    outer, inner, x_ref, c_ref, wq_hbm, wk_hbm, wv_hbm, out_ref,
    wq_ref, wk_ref, wv_ref, own_ref, up_ref, load, send_u, recv_u, send_p, recv_p,
):
    loads = []
    for n, (src, dst) in enumerate(((wq_hbm, wq_ref), (wk_hbm, wk_ref), (wv_hbm, wv_ref))):
        copy = pltpu.make_async_copy(src, dst, load.at[n])
        copy.start()
        loads.append(copy)
    size, me, where = group("seq", outer, inner)
    split = size // H
    wide = DV // split
    cut = 2 * DK + wide
    for h in range(H):
        flat = c_ref[:, h * DV : (h + 1) * DV].astype(F32).T
        for n in range(split):
            up_ref[h * split + n] = flat[n * wide : (n + 1) * wide]
    greet([(size, me, where)])
    copies = []
    for k in range(1, size):
        peer = (me + k) % size
        dst = out_ref.at[me, pl.ds(cut, wide)]
        copies.append(push(up_ref.at[peer], dst, send_u.at[k], recv_u.at[k], where(peer)))
    x = x_ref[...]
    for n, (w_ref, copy) in enumerate(zip((wq_ref, wk_ref), loads)):
        copy.wait()
        flat = dot(x, w_ref[...], (1, 0)).T
        for s in range(size):
            at = (s // split) * DK
            own_ref[s, n * DK : (n + 1) * DK, :] = flat[at : at + DK]
    loads[2].wait()
    for h in range(H):
        flat = dot(x, wv_ref[:, h * DV : (h + 1) * DV], (1, 0)).astype(BF).astype(F32).T
        for n in range(split):
            own_ref[h * split + n, 2 * DK :, :] = flat[n * wide : (n + 1) * wide]
    for k in range(1, size):
        peer = (me + k) % size
        dst = out_ref.at[me, pl.ds(0, cut)]
        copies.append(push(own_ref.at[peer], dst, send_p.at[k], recv_p.at[k], where(peer)))
    out_ref[me, :cut, :] = own_ref[me]
    out_ref[me, cut:, :] = up_ref[me]
    for copy in copies:
        copy.wait()


def front(tokens, upstream, weights, outer, inner):
    seqs = outer * inner
    length = tokens.shape[0]
    wide = DV * H // seqs
    cut = 2 * DK + wide
    scratch = [pltpu.VMEM(w.shape, w.dtype) for w in weights]
    scratch += [pltpu.VMEM((seqs, cut, length), F32), pltpu.VMEM((seqs, wide, length), F32)]
    return pl.pallas_call(
        functools.partial(front_kernel, outer, inner),
        out_shape=jax.ShapeDtypeStruct((seqs, cut + wide, length), F32),
        in_specs=[VMEM] * 2 + [HBM] * 3,
        out_specs=VMEM,
        scratch_shapes=scratch + [sems(3)] + [sems(seqs)] * 4,
        compiler_params=params(0),
    )(tokens, upstream, *weights)


def tail_kernel(
    outer, inner, pieces, g_ref, xb_ref, wq_hbm, wk_hbm, wv_hbm, gi_ref, oq_ref, ok_ref, ov_ref,
    wq_ref, wk_ref, wv_ref, jt_ref, jb_ref, gj_ref, ls_ref, lr_ref, fs_ref, os_ref, o_ref,
    load, send_j, recv_j, send_l, recv_l, send_o, recv_o,
):
    loads = []
    for n, (src, dst) in enumerate(((wq_hbm, wq_ref), (wk_hbm, wk_ref), (wv_hbm, wv_ref))):
        copy = pltpu.make_async_copy(src, dst, load.at[n])
        copy.start()
        loads.append(copy)
    plane, mine, where = group("plane", outer, inner)
    lines, high, along = group("line", outer, inner)
    _, core, sibling = group("pair", outer, inner)
    greet([(plane, mine, where), (lines, high, along), (2, core, sibling)])
    other = 1 - core
    seqs = outer * inner
    split = seqs // H
    wide = DV // split
    blocks = []
    for n in range(2):
        rows = []
        for h in range(H):
            total = g_ref[h * split, n * DK : (n + 1) * DK, :]
            for s in range(1, split):
                total = total + g_ref[h * split + s, n * DK : (n + 1) * DK, :]
            rows.append(total)
        blocks.append(jnp.concatenate(rows, 0))
    for h in range(H):
        blocks.append(
            jnp.concatenate([g_ref[h * split + s, 2 * DK :, :] for s in range(split)], 0)
        )
    for i in range(pieces):
        for half in range(2):
            jb_ref[half, i] = blocks[half * pieces + i].astype(BF).astype(F32)
    gathers = []
    for i in range(pieces):
        row = []
        for k in range(1, plane):
            peer = (mine + k) % plane
            src = jb_ref.at[peer % 2, i]
            row.append(
                push(src, gj_ref.at[i, mine], send_j.at[i, k], recv_j.at[i, k], where(peer))
            )
        gathers.append(row)
    for n, block in enumerate(blocks):
        jt_ref[:, n * DV : (n + 1) * DV] = block.T.astype(BF)
    for i in range(pieces):
        gj_ref[i, mine] = jb_ref[core, i]
    for copy in loads:
        copy.wait()
    depth = gi_ref.shape[1] // pieces // 256 * 256
    starts = [i * depth for i in range(pieces)] + [gi_ref.shape[1]]
    tokens = plane * xb_ref.shape[1]
    rows = xb_ref.shape[2] // lines
    reduces = []
    for i in range(pieces):
        cut = slice(starts[i], starts[i + 1])
        total = dot(jt_ref[:, :DV], wq_ref[cut, :], (1, 1))
        total = total + dot(jt_ref[:, DV : 2 * DV], wk_ref[cut, :], (1, 1))
        total = total + dot(jt_ref[:, 2 * DV :], wv_ref[cut, :], (1, 1))
        gi_ref[:, cut] = total.astype(BF)
        for copy in gathers[i]:
            copy.wait_recv()
        grads = jnp.concatenate([gj_ref[i, j].astype(BF) for j in range(plane)], 1)
        part = dot(grads, xb_ref[...].reshape(tokens, xb_ref.shape[2]), (1, 0))
        for z in range(lines):
            ls_ref[i, z] = part[:, z * rows : (z + 1) * rows]
        row = []
        for k in range(1, lines):
            peer = (high + k) % lines
            row.append(
                push(ls_ref.at[i, peer], lr_ref.at[i, k], send_l.at[i, k], recv_l.at[i, k], along(peer))
            )
        reduces.append(row)
    lasts = []
    keep = rows // 2
    for i in range(pieces):
        total = ls_ref[i, high]
        for k, copy in enumerate(reduces[i]):
            copy.wait_recv()
            total = total + lr_ref[i, k + 1]
        fs_ref[i] = total.T
        src = fs_ref.at[i, pl.ds(pl.multiple_of(other * keep, keep), keep)]
        lasts.append(push(src, os_ref.at[i], send_o.at[i], recv_o.at[i], sibling(other)))
        o_ref[core * pieces + i] = fs_ref[i, pl.ds(pl.multiple_of(core * keep, keep), keep), :]
    for i, copy in enumerate(lasts):
        copy.wait_recv()
        o_ref[other * pieces + i] = os_ref[i]
    oq_ref[...] = o_ref[0]
    ok_ref[...] = o_ref[1]
    for n in range(H):
        ov_ref[:, n * DV : (n + 1) * DV] = o_ref[2 + n]
    for row in gathers + reduces + [lasts]:
        for copy in row:
            copy.wait_send()


def tail(grads, inside, weights, outer, inner):
    seqs, _, length = grads.shape
    width = weights[0].shape[0]
    pieces = sum(w.shape[1] for w in weights) // (2 * DV)
    rows = width // seqs
    plane = 2 * inner
    vm = lambda *shape: pltpu.VMEM(shape, F32)
    scratch = [pltpu.VMEM(w.shape, w.dtype) for w in weights] + [
        pltpu.VMEM((length, 2 * pieces * DV), BF),
        vm(2, pieces, DV, length),
        vm(pieces, plane, DV, length),
        vm(pieces, outer, DV, rows),
        vm(pieces, outer, DV, rows),
        vm(pieces, rows, DV),
        vm(pieces, rows // 2, DV),
        vm(2 * pieces, rows // 2, DV),
        sems(3),
        sems(pieces, plane), sems(pieces, plane),
        sems(pieces, outer), sems(pieces, outer),
        sems(pieces), sems(pieces),
    ]
    return pl.pallas_call(
        functools.partial(tail_kernel, outer, inner, pieces),
        out_shape=[
            jax.ShapeDtypeStruct((length, width), BF),
            jax.ShapeDtypeStruct((rows // 2, DV), F32),
            jax.ShapeDtypeStruct((rows // 2, DV), F32),
            jax.ShapeDtypeStruct((rows // 2, H * DV), F32),
        ],
        in_specs=[VMEM] * 2 + [HBM] * 3,
        out_specs=[VMEM] * 4,
        scratch_shapes=scratch,
        compiler_params=params(2),
    )(grads, inside, *weights)


def body(inputs, cotangent, w_query, w_key, w_value):
    seqs = lax.axis_size("seq")
    outer = 4 if seqs % 4 == 0 else 1
    inner = seqs // outer
    wide = DV * H // seqs
    tokens = inputs[0]
    weights = (w_query, w_key, w_value)
    received = front(tokens, cotangent[0], weights, outer, inner)
    grads, inside = attention(received, tokens, wide, outer, inner)
    grad_in, grad_wq, grad_wk, grad_wv = tail(grads, inside, weights, outer, inner)
    return (grad_in[None], grad_wq, grad_wk, grad_wv)


def solution(mesh):
    in_specs = (P("batch", "seq", None), P("batch", "seq", None), P(), P(), P())
    out_specs = (
        P("batch", "seq", None),
        P(("seq", "batch"), None),
        P(("seq", "batch"), None),
        P(("seq", "batch"), None),
    )
    return jax.shard_map(body, mesh=mesh, in_specs=in_specs, out_specs=out_specs, check_vma=False)
```

```python
import functools
import math

import jax
import jax.numpy as jnp
import numpy as np
from jax import lax
from jax.experimental import pallas as pl
from jax.experimental.pallas import tpu as pltpu
from jax.sharding import PartitionSpec as P

H = 8
DK = 16
DV = 128
AUX = 16
MESH = pl.DeviceIdType.MESH
BF = jnp.bfloat16
F32 = jnp.float32


def group(kind, outer, inner):
    seq = lax.axis_index("seq")
    core = lax.axis_index("batch")
    high = seq // inner
    low = seq % inner
    if kind == "seq":
        return outer * inner, seq, lambda j: (j, core)
    if kind == "plane":
        return inner * 2, low * 2 + core, lambda j: (high * inner + j // 2, j % 2)
    if kind == "line":
        return outer, high, lambda j: (j * inner + low, core)
    if kind == "chips":
        return inner, low, lambda j: (high * inner + j, core)
    return 2, core, lambda j: (seq, j)


def greet(groups):
    barrier = pltpu.get_barrier_semaphore()
    total = 0
    for size, me, where in groups:
        for k in range(1, size):
            pl.semaphore_signal(
                barrier, inc=1, device_id=where((me + k) % size), device_id_type=MESH
            )
        total += size - 1
    pl.semaphore_wait(barrier, total)


def push(src, dst, send, recv, device):
    copy = pltpu.make_async_remote_copy(
        src_ref=src,
        dst_ref=dst,
        send_sem=send,
        recv_sem=recv,
        device_id=device,
        device_id_type=MESH,
    )
    copy.start()
    return copy


VMEM = pl.BlockSpec(memory_space=pltpu.VMEM)
HBM = pl.BlockSpec(memory_space=pl.ANY)


def sems(*sizes):
    return pltpu.SemaphoreType.DMA(sizes)


def params(number):
    return pltpu.CompilerParams(
        collective_id=number, has_side_effects=True, vmem_limit_bytes=60 << 20
    )


def dot(left, right, dims):
    return lax.dot_general(left, right, ((dims[:1], dims[1:]), ((), ())), preferred_element_type=F32)


def halves(a):
    high = a.astype(BF)
    return high, (a - high.astype(F32)).astype(BF)


def dot2(pair, right, dims):
    return dot(pair[0], right, dims) + dot(pair[1], right, dims)


def dot2r(left, pair, dims):
    return dot(left, pair[0], dims) + dot(left, pair[1], dims)


def dot3(lefts, rights, dims):
    return (
        dot(lefts[0], rights[0], dims)
        + dot(lefts[0], rights[1], dims)
        + dot(lefts[1], rights[0], dims)
    )


def coefs():
    table = np.where(np.eye(DK) > 0, 1.0 / math.sqrt(2.0), 1.0).astype(np.float32)
    table = table * (np.arange(DK)[:, None] <= np.arange(DK)[None, :])
    half = DK // 2
    rows = np.concatenate([table[:half].reshape(-1), table[half:, half:].reshape(-1)])
    return np.ascontiguousarray(np.broadcast_to(rows[:, None], (rows.size, 128)))


def phi(u, coef):
    half = DK // 2
    lanes = u.shape[1]
    pieces = []
    for i in range(DK):
        low = u if i < half else u[half:]
        pieces.append(u[i : i + 1] * low)
    pairs = jnp.concatenate(pieces, 0) * coef
    first = (lax.broadcasted_iota(jnp.int32, (AUX, lanes), 0) == 0).astype(F32)
    return jnp.concatenate([pairs, u, first], 0)


def pull(u, grad, coef):
    half = DK // 2
    pairs = grad[: coef.shape[0]] * coef
    linear = grad[coef.shape[0] : coef.shape[0] + DK]
    rows = lax.broadcasted_iota(jnp.int32, u.shape, 0)
    total = linear
    lower = jnp.zeros_like(u[half:])
    at = 0
    for i in range(DK):
        if i < half:
            piece = pairs[at : at + DK]
            at += DK
            total = total + piece * u[i : i + 1]
            mine = jnp.sum(piece * u, 0, keepdims=True)
        else:
            piece = pairs[at : at + half]
            at += half
            lower = lower + piece * u[i : i + 1]
            mine = jnp.sum(piece * u[half:], 0, keepdims=True)
        total = total + jnp.where(rows == i, mine, 0.0)
    return total + jnp.concatenate([jnp.zeros_like(lower), lower], 0)


def attention_kernel(
    wide, outer, inner, r_ref, c_ref, x_ref, got_ref, xb_ref,
    o_ref, fq_ref, fk_ref, va_ref, ah, al, gh, gl, nh, nl, st_ref, gi_ref, pg_ref,
    send_i, recv_i, send_x, recv_x, send_q, recv_q, send_r, recv_r,
):
    blocks, _, tokens = r_ref.shape
    size, me, where = group("seq", outer, inner)
    chips, low, chip = group("chips", outer, inner)
    _, core, sibling = group("pair", outer, inner)
    rows = st_ref.shape[2] // outer
    for j in range(inner):
        for z in range(outer):
            at = (z * inner + j) * rows
            st_ref[j, :, z * rows : (z + 1) * rows] = x_ref[:, at : at + rows].astype(F32)
    greet([(size, me, where), (chips, low, chip), (2, core, sibling)])
    inside = []
    for k in range(1, chips):
        peer = (low + k) % chips
        inside.append(
            push(st_ref.at[peer], gi_ref.at[low], send_i.at[k], recv_i.at[k], chip(peer))
        )
    gi_ref[low] = st_ref[low]
    length = 2 * tokens
    chunks = blocks // 2
    feats = fq_ref.shape[1]
    coef = jnp.concatenate([c_ref[...]] * (length // 128), 1)
    causal = lax.broadcasted_iota(jnp.int32, (length, length), 0) <= lax.broadcasted_iota(
        jnp.int32, (length, length), 1
    )
    aux_row = lax.broadcasted_iota(jnp.int32, (AUX, length), 0) == 0

    def block(c):
        return jnp.concatenate([r_ref[2 * c], r_ref[2 * c + 1]], 1)

    def store(c, start, rows):
        size = rows.shape[0]
        o_ref[2 * c, start : start + size, :] = rows[:, :tokens]
        o_ref[2 * c + 1, start : start + size, :] = rows[:, tokens:]

    def forward(c, state):
        both = block(c)
        uq = both[:DK] * 0.5
        uk = both[DK : 2 * DK] * 0.5
        val = both[2 * DK : 2 * DK + wide]
        up = both[2 * DK + wide :]
        fq = phi(uq, coef).astype(BF)
        fk = phi(uk, coef).astype(BF)
        va = jnp.concatenate([val, aux_row.astype(F32)], 0).astype(BF)
        fq_ref[c] = fq
        fk_ref[c] = fk
        va_ref[c] = va
        attn = halves(jnp.where(causal, dot(fk, fq, (0, 0)), 0.0))
        ah[c] = attn[0]
        al[c] = attn[1]
        held = halves(state)
        top = dot2r(va, attn, (1, 0)) + dot2(held, fq, (1, 0))
        scale = 1.0 / top[wide : wide + 1]
        numer = up * scale
        denom = -jnp.sum(numer * top[:wide], 0, keepdims=True) * scale
        gn = halves(jnp.concatenate([numer, jnp.where(aux_row, denom, 0.0)], 0))
        nh[c] = gn[0]
        nl[c] = gn[1]
        ga = halves(jnp.where(causal, dot2r(va, gn, (0, 0)), 0.0))
        gh[c] = ga[0]
        gl[c] = ga[1]
        gfq = dot2r(fk, ga, (1, 0)) + dot3(held, gn, (0, 0))
        store(c, 0, pull(uq, gfq, coef) * 0.5)
        return state + dot(va, fk, (1, 1))

    zero = jnp.zeros((wide + AUX, feats), F32)
    lax.fori_loop(0, chunks, forward, zero)

    def give(start, count, send, recv):
        copies = []
        for k in range(1, size):
            peer = (me + k) % size
            src = o_ref.at[peer, pl.ds(start, count)]
            dst = got_ref.at[me, pl.ds(start, count)]
            copies.append(push(src, dst, send.at[k], recv.at[k], where(peer)))
        return copies

    returns = give(0, DK, send_q, recv_q)

    def backward(step, state):
        c = chunks - 1 - step
        uk = block(c)[DK : 2 * DK] * 0.5
        fq, fk, va = fq_ref[c], fk_ref[c], va_ref[c]
        attn = (ah[c], al[c])
        ga = (gh[c], gl[c])
        gn = (nh[c], nl[c])
        held = halves(state)
        gv = dot3(gn, attn, (1, 1)) + dot2(held, fk, (1, 0))
        store(c, 2 * DK, gv[:wide])
        gfk = dot2r(fq, ga, (1, 1)) + dot2(held, va, (0, 0))
        store(c, DK, pull(uk, gfk, coef) * 0.5)
        return state + dot2(gn, fq, (1, 1))

    lax.fori_loop(0, chunks, backward, zero)
    returns += give(DK, DK + wide, send_r, recv_r)
    got_ref[me] = o_ref[me]
    for copy in inside:
        copy.wait()
    pair = push(gi_ref, pg_ref, send_x.at[0], recv_x.at[0], sibling(1 - core))
    for j in range(inner):
        xb_ref[2 * j + core] = gi_ref[j].astype(BF)
    pair.wait()
    for j in range(inner):
        xb_ref[2 * j + 1 - core] = pg_ref[j].astype(BF)
    for copy in returns:
        copy.wait()


def attention(received, tokens_in, wide, outer, inner):
    blocks, _, tokens = received.shape
    coef = coefs()
    feats = coef.shape[0] + DK + AUX
    chunks, length = blocks // 2, 2 * tokens
    width = tokens_in.shape[1] // inner
    square = pltpu.VMEM((chunks, length, length), BF)
    grads = pltpu.VMEM((chunks, wide + AUX, length), BF)
    feat = pltpu.VMEM((chunks, feats, length), BF)
    result = (blocks, 2 * DK + wide, tokens)
    group_in = pltpu.VMEM((inner, tokens, width), F32)
    scratch = [pltpu.VMEM(result, F32), feat, feat, grads, square, square, square, square]
    scratch += [grads, grads, group_in, group_in, group_in]
    scratch += [sems(inner)] * 2 + [sems(1)] * 2 + [sems(blocks)] * 4
    return pl.pallas_call(
        functools.partial(attention_kernel, wide, outer, inner),
        out_shape=[
            jax.ShapeDtypeStruct(result, F32),
            jax.ShapeDtypeStruct((2 * inner, tokens, width), BF),
        ],
        in_specs=[VMEM] * 3,
        out_specs=[VMEM] * 2,
        scratch_shapes=scratch,
        compiler_params=params(1),
    )(received, jnp.asarray(coef), tokens_in)


def front_kernel(
    outer, inner, x_ref, c_ref, wq_hbm, wk_hbm, wv_hbm, out_ref,
    wq_ref, wk_ref, wv_ref, own_ref, up_ref, load, send_u, recv_u, send_p, recv_p,
):
    loads = []
    for n, (src, dst) in enumerate(((wq_hbm, wq_ref), (wk_hbm, wk_ref), (wv_hbm, wv_ref))):
        copy = pltpu.make_async_copy(src, dst, load.at[n])
        copy.start()
        loads.append(copy)
    size, me, where = group("seq", outer, inner)
    split = size // H
    wide = DV // split
    cut = 2 * DK + wide
    for h in range(H):
        flat = c_ref[:, h * DV : (h + 1) * DV].astype(F32).T
        for n in range(split):
            up_ref[h * split + n] = flat[n * wide : (n + 1) * wide]
    greet([(size, me, where)])
    copies = []
    for k in range(1, size):
        peer = (me + k) % size
        dst = out_ref.at[me, pl.ds(cut, wide)]
        copies.append(push(up_ref.at[peer], dst, send_u.at[k], recv_u.at[k], where(peer)))
    x = x_ref[...]
    for n, (w_ref, copy) in enumerate(zip((wq_ref, wk_ref), loads)):
        copy.wait()
        flat = dot(x, w_ref[...], (1, 0)).T
        for s in range(size):
            at = (s // split) * DK
            own_ref[s, n * DK : (n + 1) * DK, :] = flat[at : at + DK]
    loads[2].wait()
    for h in range(H):
        flat = dot(x, wv_ref[:, h * DV : (h + 1) * DV], (1, 0)).astype(BF).astype(F32).T
        for n in range(split):
            own_ref[h * split + n, 2 * DK :, :] = flat[n * wide : (n + 1) * wide]
    for k in range(1, size):
        peer = (me + k) % size
        dst = out_ref.at[me, pl.ds(0, cut)]
        copies.append(push(own_ref.at[peer], dst, send_p.at[k], recv_p.at[k], where(peer)))
    out_ref[me, :cut, :] = own_ref[me]
    out_ref[me, cut:, :] = up_ref[me]
    for copy in copies:
        copy.wait()


def front(tokens, upstream, weights, outer, inner):
    seqs = outer * inner
    length = tokens.shape[0]
    wide = DV * H // seqs
    cut = 2 * DK + wide
    scratch = [pltpu.VMEM(w.shape, w.dtype) for w in weights]
    scratch += [pltpu.VMEM((seqs, cut, length), F32), pltpu.VMEM((seqs, wide, length), F32)]
    return pl.pallas_call(
        functools.partial(front_kernel, outer, inner),
        out_shape=jax.ShapeDtypeStruct((seqs, cut + wide, length), F32),
        in_specs=[VMEM] * 2 + [HBM] * 3,
        out_specs=VMEM,
        scratch_shapes=scratch + [sems(3)] + [sems(seqs)] * 4,
        compiler_params=params(0),
    )(tokens, upstream, *weights)


def tail_kernel(
    outer, inner, pieces, g_ref, xb_ref, wq_hbm, wk_hbm, wv_hbm, gi_ref, o_ref,
    wq_ref, wk_ref, wv_ref, jt_ref, jb_ref, gj_ref, ls_ref, lr_ref, fs_ref, os_ref,
    load, send_j, recv_j, send_l, recv_l, send_o, recv_o,
):
    loads = []
    for n, (src, dst) in enumerate(((wq_hbm, wq_ref), (wk_hbm, wk_ref), (wv_hbm, wv_ref))):
        copy = pltpu.make_async_copy(src, dst, load.at[n])
        copy.start()
        loads.append(copy)
    plane, mine, where = group("plane", outer, inner)
    lines, high, along = group("line", outer, inner)
    _, core, sibling = group("pair", outer, inner)
    greet([(plane, mine, where), (lines, high, along), (2, core, sibling)])
    other = 1 - core
    seqs = outer * inner
    split = seqs // H
    wide = DV // split
    blocks = []
    for n in range(2):
        rows = []
        for h in range(H):
            total = g_ref[h * split, n * DK : (n + 1) * DK, :]
            for s in range(1, split):
                total = total + g_ref[h * split + s, n * DK : (n + 1) * DK, :]
            rows.append(total)
        blocks.append(jnp.concatenate(rows, 0))
    for h in range(H):
        blocks.append(
            jnp.concatenate([g_ref[h * split + s, 2 * DK :, :] for s in range(split)], 0)
        )
    for i in range(pieces):
        for half in range(2):
            jb_ref[half, i] = blocks[half * pieces + i].astype(BF).astype(F32)
    gathers = []
    for i in range(pieces):
        row = []
        for k in range(1, plane):
            peer = (mine + k) % plane
            src = jb_ref.at[peer % 2, i]
            row.append(
                push(src, gj_ref.at[i, mine], send_j.at[i, k], recv_j.at[i, k], where(peer))
            )
        gathers.append(row)
    for n, block in enumerate(blocks):
        jt_ref[:, n * DV : (n + 1) * DV] = block.T.astype(BF)
    for i in range(pieces):
        gj_ref[i, mine] = jb_ref[core, i]
    for copy in loads:
        copy.wait()
    depth = gi_ref.shape[1] // pieces // 256 * 256
    starts = [i * depth for i in range(pieces)] + [gi_ref.shape[1]]
    tokens = plane * xb_ref.shape[1]
    rows = xb_ref.shape[2] // lines
    reduces = []
    for i in range(pieces):
        cut = slice(starts[i], starts[i + 1])
        total = dot(jt_ref[:, :DV], wq_ref[cut, :], (1, 1))
        total = total + dot(jt_ref[:, DV : 2 * DV], wk_ref[cut, :], (1, 1))
        total = total + dot(jt_ref[:, 2 * DV :], wv_ref[cut, :], (1, 1))
        gi_ref[:, cut] = total.astype(BF)
        for copy in gathers[i]:
            copy.wait_recv()
        grads = jnp.concatenate([gj_ref[i, j].astype(BF) for j in range(plane)], 1)
        part = dot(grads, xb_ref[...].reshape(tokens, xb_ref.shape[2]), (1, 0))
        for z in range(lines):
            ls_ref[i, z] = part[:, z * rows : (z + 1) * rows]
        row = []
        for k in range(1, lines):
            peer = (high + k) % lines
            row.append(
                push(ls_ref.at[i, peer], lr_ref.at[i, k], send_l.at[i, k], recv_l.at[i, k], along(peer))
            )
        reduces.append(row)
    lasts = []
    keep = rows // 2
    for i in range(pieces):
        total = ls_ref[i, high]
        for k, copy in enumerate(reduces[i]):
            copy.wait_recv()
            total = total + lr_ref[i, k + 1]
        fs_ref[i] = total.T
        src = fs_ref.at[i, pl.ds(pl.multiple_of(other * keep, keep), keep)]
        lasts.append(push(src, os_ref.at[i], send_o.at[i], recv_o.at[i], sibling(other)))
        o_ref[core * pieces + i] = fs_ref[i, pl.ds(pl.multiple_of(core * keep, keep), keep), :]
    for i, copy in enumerate(lasts):
        copy.wait_recv()
        o_ref[other * pieces + i] = os_ref[i]
    for row in gathers + reduces + [lasts]:
        for copy in row:
            copy.wait_send()


def tail(grads, inside, weights, outer, inner):
    seqs, _, length = grads.shape
    width = weights[0].shape[0]
    pieces = sum(w.shape[1] for w in weights) // (2 * DV)
    rows = width // seqs
    plane = 2 * inner
    vm = lambda *shape: pltpu.VMEM(shape, F32)
    scratch = [pltpu.VMEM(w.shape, w.dtype) for w in weights] + [
        pltpu.VMEM((length, 2 * pieces * DV), BF),
        vm(2, pieces, DV, length),
        vm(pieces, plane, DV, length),
        vm(pieces, outer, DV, rows),
        vm(pieces, outer, DV, rows),
        vm(pieces, rows, DV),
        vm(pieces, rows // 2, DV),
        sems(3),
        sems(pieces, plane), sems(pieces, plane),
        sems(pieces, outer), sems(pieces, outer),
        sems(pieces), sems(pieces),
    ]
    return pl.pallas_call(
        functools.partial(tail_kernel, outer, inner, pieces),
        out_shape=[
            jax.ShapeDtypeStruct((length, width), BF),
            jax.ShapeDtypeStruct((2 * pieces, rows // 2, DV), F32),
        ],
        in_specs=[VMEM] * 2 + [HBM] * 3,
        out_specs=[VMEM] * 2,
        scratch_shapes=scratch,
        compiler_params=params(2),
    )(grads, inside, *weights)


def finish_kernel(gi_ref, o_ref, in_ref, oq_ref, ok_ref, ov_ref):
    in_ref[0] = gi_ref[...]
    oq_ref[...] = o_ref[0]
    ok_ref[...] = o_ref[1]
    for n in range(H):
        ov_ref[:, n * DV : (n + 1) * DV] = o_ref[2 + n]


def finish(grad_in, blocks):
    _, rows, lanes = blocks.shape
    return pl.pallas_call(
        finish_kernel,
        out_shape=[
            jax.ShapeDtypeStruct((1,) + grad_in.shape, BF),
            jax.ShapeDtypeStruct((rows, lanes), F32),
            jax.ShapeDtypeStruct((rows, lanes), F32),
            jax.ShapeDtypeStruct((rows, H * lanes), F32),
        ],
        in_specs=[VMEM] * 2,
        out_specs=[VMEM] * 4,
    )(grad_in, blocks)


def body(inputs, cotangent, w_query, w_key, w_value):
    seqs = lax.axis_size("seq")
    outer = 4 if seqs % 4 == 0 else 1
    inner = seqs // outer
    wide = DV * H // seqs
    tokens = inputs[0]
    weights = (w_query, w_key, w_value)
    received = front(tokens, cotangent[0], weights, outer, inner)
    grads, inside = attention(received, tokens, wide, outer, inner)
    return tuple(finish(*tail(grads, inside, weights, outer, inner)))


def solution(mesh):
    in_specs = (P("batch", "seq", None), P("batch", "seq", None), P(), P(), P())
    out_specs = (
        P("batch", "seq", None),
        P(("seq", "batch"), None),
        P(("seq", "batch"), None),
        P(("seq", "batch"), None),
    )
    return jax.shard_map(body, mesh=mesh, in_specs=in_specs, out_specs=out_specs, check_vma=False)
```
